32 devices in a mesh: rows: 4 (over y, x), mp: 8 (over z, core).
Axes of the slice: x: 2, y: 2, z: 4, core: 2. Of those that a mesh axis runs over, the one named last changes fastest.
Arguments:
- tokens: bfloat16 [512, 6144], P('rows', 'mp'), may hold values from -8 to 8
- norm_gain: float32 [6144], replicated, may hold values from 0.25 to 1.75
- hidden_bias: float32 [24576], P('mp'), may hold values from -3 to 3
- weight_in: bfloat16 [6144, 24576], P('rows', 'mp'), may hold values from -0.078125 to 0.078125
- weight_out: bfloat16 [24576, 6144], P('mp', 'rows'), may hold values from -0.0546875 to 0.0546875
Outputs:
- updated: bfloat16 [512, 6144], P('rows', 'mp')
The draws below stay inside these ranges and needn't reach their ends.
All inputs are finite; a program needn't handle non-finite values.
Results may differ from the reference program's by a relative error of at most 0.0041.
Values may be sent and summed in bfloat16 or wider, within the bound.
A program may use at most 128 MiB of HBM per device.

```python
import jax
import jax.numpy as jnp
from jax import lax

D = 6144
FF = 24576
TOKENS = 512


def raised(array, own_key, source, target, blocks, factor):
    owner, partner = [(jnp.arange(array.shape[position]) // (array.shape[position] // blocks)).reshape([-1 if axis == position else 1 for axis in range(array.ndim)]) for position in (source, target)]
    chosen = jax.random.permutation(own_key, blocks)[partner]
    strong = (owner == chosen) | (owner == (partner + blocks // 2) % blocks)
    return jnp.where(strong, factor * array, array)


def block_scale(own_key, extent, cuts, smallest, high):
    factor_of = 1.0
    for dim, blocks in cuts:
        heights = jax.random.uniform(jax.random.fold_in(jax.random.fold_in(own_key, 6), dim), (blocks,), jnp.float32, smallest / len(cuts), high / len(cuts))
        factor_of = factor_of * jnp.repeat(jnp.exp(heights), extent[dim] // blocks).reshape((-1,) + (1,) * (len(extent) - 1 - dim))
    return factor_of


def gaussian(own_key, extent, spread, limit, split=(), dtype=jnp.bfloat16):
    array = spread * jax.random.normal(own_key, extent, jnp.float32)
    if split:
        array = array * block_scale(own_key, extent, split, -0.22, 0.18)
    return jnp.clip(array, -limit, limit).astype(dtype)


def heavy_noise(stream_key, extent, spread, reach, shards, heavy, kind=jnp.bfloat16):
    array = spread * jax.random.normal(stream_key, extent, jnp.float32)
    if shards:
        array = array * block_scale(stream_key, extent, shards, -0.22, 0.18)
    return jnp.clip(raised(array, jax.random.fold_in(stream_key, 3), *heavy), -reach, reach).astype(kind)


def setup_inputs(seed: int = 0) -> dict:
    streams_of = jax.random.split(jax.random.key(seed), 6)
    return {
        "tokens": heavy_noise(streams_of[0], (TOKENS, D), 1.0, 8.0, ((0, 4), (1, 8)), (1, 0, 8, 2.0)),
        "norm_gain": jnp.clip(1.0 + 0.15 * jax.random.normal(streams_of[1], (D,), jnp.float32), 0.25, 1.75),
        "hidden_bias": gaussian(streams_of[2], (FF,), 0.5, 3.0, ((0, 8),), jnp.float32),
        "weight_in": gaussian(streams_of[3], (D, FF), D ** -0.5, 0.078125, ((0, 4), (1, 8))),
        "weight_out": heavy_noise(streams_of[4], (FF, D), FF ** -0.5, 0.0546875, ((0, 8), (1, 4)), (0, 1, 8, 2.0)),
    }


floor_value = 0.1

def normalize(as_float, moment_sum, square_sum, gain, width):
    row_mean = moment_sum / width
    row_var = jnp.maximum(square_sum / width - row_mean * row_mean, 0.0)
    inverse = lax.rsqrt(row_var + floor_value)
    return ((as_float - row_mean[:, None]) * inverse[:, None] * gain[None, :]).astype(jnp.bfloat16)

def reference(tokens, norm_gain, hidden_bias, weight_in, weight_out):
    as_float = tokens.astype(jnp.float32)
    normed = normalize(as_float, lax.optimization_barrier(jnp.sum(as_float, axis=1)), lax.optimization_barrier(jnp.sum(as_float * as_float, axis=1)), norm_gain, D)
    preact = jnp.dot(normed, weight_in, preferred_element_type=jnp.float32) + hidden_bias[None, :]
    hidden = jax.nn.gelu(preact, approximate=False).astype(jnp.bfloat16)
    branch = jnp.dot(hidden, weight_out, preferred_element_type=jnp.float32)
    return (as_float + branch).astype(jnp.bfloat16)
```

```python
import functools

import jax
import jax.numpy as jnp
from jax import lax
from jax.experimental import pallas as pl
from jax.experimental.pallas import tpu as pltpu
from jax.sharding import PartitionSpec as P

MESH = pl.DeviceIdType.MESH
F32 = jnp.float32
BF16 = jnp.bfloat16
floor_value = 0.1
UNITS = (1, 2, 2, 2, 1)


def gelu(x):
    return 0.5 * x * (1.0 + lax.erf(x * 0.7071067811865476))


def kernel(
    R, M, D, cuts, order, tok, gain, bias, win_hbm, wout_hbm, out, win, wout, xs, nx, stc, mi, colst,
    pbuf, r1, r2, qbuf, hid, osend, osib, oown, csend, cmid, crecv, wsem,
    s_a, r_a, s_sib, r_sib, s_st, r_st, s_mi, r_mi, s_r1, r_r1, s_r2, r_r2, s_ag, r_ag, s_os, r_os,
    s_cm, r_cm, s_cz, r_cz,
):
    r = lax.axis_index("rows")
    m = lax.axis_index("mp")
    Z = M // 2
    z, c = m // 2, m % 2
    sib = 2 * z + 1 - c
    height, width = tok.shape
    half = win.shape[1] // 2
    K = len(cuts)
    offs = [sum(cuts[:k]) for k in range(K)]
    rx, ry, rd = r + 1 - 2 * (r % 2), (r + 2) % 4, 3 - r
    first, second = (rx, ry), (ry, rx)
    peers = (rd, rx, ry)
    home = z == r

    pltpu.make_async_copy(win_hbm, win, wsem.at[0]).start()
    pltpu.make_async_copy(wout_hbm, wout, wsem.at[1]).start()

    def remote(src, dst, ssem, rsem, row, col):
        return pltpu.make_async_remote_copy(
            src_ref=src, dst_ref=dst, send_sem=ssem, recv_sem=rsem, device_id=(row, col), device_id_type=MESH
        )

    def part(k):
        return pl.ds(offs[k], cuts[k])

    barrier = pltpu.get_barrier_semaphore()

    def greet(row, col):
        pl.semaphore_signal(barrier, inc=1, device_id=(row, col), device_id_type=MESH)

    for i in range(1, M):
        greet(r, (m + i) % M)
    for i in range(1, R):
        greet((r + i) % R, m)

    @pl.when(jnp.logical_not(home))
    def _():
        for i in range(1, R):
            greet((r + i) % R, 2 * r + c)

    own = tok[...].astype(F32)
    lane = lax.broadcasted_iota(jnp.int32, (height, 128), 1)
    s1 = jnp.sum(own, axis=1, keepdims=True)
    s2 = jnp.sum(own * own, axis=1, keepdims=True)
    stc[m] = jnp.where(lane == 0, s1, s2).T[0:8]

    pl.semaphore_wait(barrier, (M - 1) + (R - 1) + jnp.where(home, 0, R - 1))

    toward = 2 * (z // 2) - 1

    def c_a(k, i):
        zd = (z + i * toward + Z) % Z
        return remote(tok.at[part(k)], xs.at[c, r, part(k)], s_a.at[k, i], r_a.at[k, r], z, 2 * zd + c)

    def c_sib(k, t, src):
        return remote(src, xs.at[c, t, part(k)], s_sib.at[k, t], r_sib.at[k, t], r, sib)

    def c_st(i):
        return remote(stc.at[m], stc.at[m], s_st.at[i], r_st.at[m], r, (m + i) % M)

    def c_mi(i):
        return remote(mi.at[r], mi.at[r], s_mi.at[i], r_mi.at[r], peers[i], m)

    def c_r1(k, h, i):
        tile = (first[h], rd)[i]
        return remote(
            pbuf.at[h, tile, part(k)], r1.at[h, i, part(k)], s_r1.at[k, h, i], r_r1.at[k, h, i], first[h], m
        )

    def c_r2(k, h):
        return remote(qbuf.at[h, part(k)], r2.at[h, part(k)], s_r2.at[k, h], r_r2.at[k, h], second[h], m)

    def c_ag(k, h, i):
        tile = (r, r, second[h])[i]
        to = (second[h], first[h], first[h])[i]
        ref = hid.at[h, tile, part(k)]
        return remote(ref, ref, s_ag.at[k, h, i], r_ag.at[k, h, tile], to, m)

    def w_ag(k, h, tile):
        ref = hid.at[h, tile, part(k)]
        return remote(ref, ref, s_ag.at[k, h, 0], r_ag.at[k, h, tile], first[h], m)

    def c_os(k):
        return remote(osend.at[:, part(k)], osib.at[:, part(k)], s_os.at[k], r_os.at[k], r, sib)

    def c_cm(k, i):
        t = peers[i]
        return remote(csend.at[t, part(k)], cmid.at[r, part(k)], s_cm.at[k, i], r_cm.at[k, r], t, m)

    def c_cz(k, q, src):
        return remote(src, crecv.at[z, part(k)], s_cz.at[k, q], r_cz.at[k, z], r, 2 * q + c)

    def stage_send(k):
        for i in range(1, Z):
            c_a(k, i).start()

        @pl.when(home)
        def _():
            xs[c, r, part(k)] = tok[part(k)]
            c_sib(k, r, tok.at[part(k)]).start()

        @pl.when(jnp.logical_not(home))
        def _():
            c_a(k, 0).start()

    def stage_st0(_):
        for i in range(1, M):
            c_st(i).start()

    def stage_st1(_):
        for i in range(1, M):
            q = (m + i) % M
            remote(stc.at[q], stc.at[q], s_st.at[i], r_st.at[q], r, q).wait_recv()
        tot = stc[0]
        for q in range(1, M):
            tot = tot + stc[q]
        mean = tot[0:1] / D
        var = jnp.maximum(tot[1:2] / D - mean * mean, 0.0)
        inv = lax.rsqrt(var + floor_value)
        sub = lax.broadcasted_iota(jnp.int32, (8, height), 0)
        mi[r] = jnp.where(sub == 0, mean, inv)
        for i in range(3):
            c_mi(i).start()

    def stage_st2(_):
        for i in range(3):
            p = peers[i]
            remote(mi.at[p], mi.at[p], s_mi.at[i], r_mi.at[p], p, m).wait_recv()
        sub = lax.broadcasted_iota(jnp.int32, (128, height), 0)
        for t in range(R):
            colst[t] = jnp.where(sub == 0, mi[t, 0:1], mi[t, 1:2]).T

    def stage_a(k):
        for i in range(R):
            t = (r + i) % R
            if i == 0:
                @pl.when(jnp.logical_not(home))
                def _():
                    remote(tok.at[part(k)], xs.at[c, r, part(k)], s_a.at[k, 0], r_a.at[k, r], r, sib).wait_recv()
                    c_sib(k, r, xs.at[c, r, part(k)]).start()
            else:
                remote(tok.at[part(k)], xs.at[c, t, part(k)], s_a.at[k, 0], r_a.at[k, t], r, sib).wait_recv()
                c_sib(k, t, xs.at[c, t, part(k)]).start()

    def stage_m1(k):
        n = cuts[k]
        for t in range(R):
            ref = xs.at[1 - c, t, part(k)]
            remote(ref, ref, s_sib.at[k, t], r_sib.at[k, t], r, sib).wait_recv()
        stats = colst[:, part(k)].reshape(R * n, 128)
        mean_c, inv_c = stats[:, 0:1], stats[:, 1:2]
        for cc in range(2):
            x = xs[cc, :, part(k)].astype(F32).reshape(R * n, width)
            nx[cc, 0:R * n] = ((x - mean_c) * inv_c * gain[2 * r + cc]).astype(BF16)

        if k == 0:
            pltpu.make_async_copy(win_hbm, win, wsem.at[0]).wait()

        tile = half // 2
        for h in range(2):
            def col(j, _):
                at = pl.multiple_of(j * tile, 128)
                wat = pl.multiple_of(h * half + j * tile, 128)
                acc = jnp.dot(nx[0, 0:R * n], win[0:width, pl.ds(wat, tile)], preferred_element_type=F32)
                acc += jnp.dot(nx[1, 0:R * n], win[width:2 * width, pl.ds(wat, tile)], preferred_element_type=F32)
                pbuf[h, :, part(k), pl.ds(at, tile)] = acc.astype(BF16).reshape(R, n, tile)
                return 0

            lax.fori_loop(0, 2, col, 0)
            c_r1(k, h, 1).start()
            c_r1(k, h, 0).start()

    def stage_b1(k):
        for h in range(2):
            c_r1(k, h, 1).wait_recv()
            mine = pbuf[h, second[h], part(k)].astype(F32)
            qbuf[h, part(k)] = (mine + r1[h, 1, part(k)].astype(F32)).astype(BF16)
            c_r2(k, h).start()

    def stage_b2(k):
        for h in range(2):
            c_r1(k, h, 0).wait_recv()
            c_r2(k, h).wait_recv()
            pre = pbuf[h, r, part(k)].astype(F32) + r1[h, 0, part(k)].astype(F32) + r2[h, part(k)].astype(F32)
            pre = pre + bias[0:1, h * half:(h + 1) * half]
            hid[h, r, part(k)] = gelu(pre).astype(BF16)
            c_ag(k, h, 0).start()
            c_ag(k, h, 1).start()

    def stage_b3(k):
        for h in range(2):
            w_ag(k, h, second[h]).wait_recv()
            c_ag(k, h, 2).start()

    def stage_b4(k):
        n = cuts[k]
        for h in range(2):
            w_ag(k, h, first[h]).wait_recv()
            w_ag(k, h, rd).wait_recv()

        if k == 0:
            pltpu.make_async_copy(wout_hbm, wout, wsem.at[1]).wait()

        def product(cc):
            at = pl.multiple_of(cc * width, 128)
            acc = None
            for h in range(2):
                a = hid[h, :, part(k)].reshape(R * n, half)
                term = jnp.dot(a, wout[h * half:(h + 1) * half, pl.ds(at, width)], preferred_element_type=F32)
                acc = term if acc is None else acc + term
            return acc.reshape(R, n, width)

        osend[:, part(k)] = product(1 - c).astype(BF16)
        c_os(k).start()
        oown[:, part(k)] = product(c)

    def stage_c1(k):
        c_os(k).wait_recv()
        csend[:, part(k)] = (oown[:, part(k)] + osib[:, part(k)].astype(F32)).astype(BF16)
        for i in range(3):
            c_cm(k, i).start()

        @pl.when(jnp.logical_not(home))
        def _():
            c_cz(k, r, csend.at[r, part(k)]).start()

    def stage_c2(k):
        for i in (1, 2, 0):
            q = peers[i]
            remote(csend.at[r, part(k)], cmid.at[q, part(k)], s_cm.at[k, i], r_cm.at[k, q], q, m).wait_recv()

            @pl.when(q != z)
            def _():
                c_cz(k, q, cmid.at[q, part(k)]).start()

    def stage_c3(k):
        @pl.when(home)
        def _():
            crecv[z, part(k)] = csend[r, part(k)]

        @pl.when(jnp.logical_not(home))
        def _():
            crecv[z, part(k)] = cmid[z, part(k)]

        for i in range(1, Z):
            q = (z + i) % Z
            ref = crecv.at[q, part(k)]
            remote(ref, ref, s_cz.at[k, 0], r_cz.at[k, q], r, sib).wait_recv()
        total = (crecv[0, part(k)].astype(F32) + crecv[1, part(k)].astype(F32)) + (
            crecv[2, part(k)].astype(F32) + crecv[3, part(k)].astype(F32)
        )
        out[part(k)] = (tok[part(k)].astype(F32) + total).astype(BF16)

    stages = {
        "send": stage_send, "st0": stage_st0, "st1": stage_st1, "st2": stage_st2, "a": stage_a, "m1": stage_m1,
        "b1": stage_b1, "b2": stage_b2, "b3": stage_b3, "b4": stage_b4, "c1": stage_c1, "c2": stage_c2, "c3": stage_c3,
    }
    for name, k in order:
        stages[name](k)

    for i in range(1, M):
        c_st(i).wait_send()
    for i in range(3):
        c_mi(i).wait_send()
    for k in range(K):
        for i in range(1, Z):
            c_a(k, i).wait_send()

        @pl.when(jnp.logical_not(home))
        def _():
            c_a(k, 0).wait_send()
            c_cz(k, r, csend.at[r, part(k)]).wait_send()

        for t in range(R):
            c_sib(k, t, xs.at[c, t, part(k)]).wait_send()
        for h in range(2):
            c_r1(k, h, 0).wait_send()
            c_r1(k, h, 1).wait_send()
            c_r2(k, h).wait_send()
            for i in range(3):
                c_ag(k, h, i).wait_send()
        c_os(k).wait_send()
        for i in range(3):
            c_cm(k, i).wait_send()
            q = peers[i]

            @pl.when(q != z)
            def _():
                c_cz(k, q, cmid.at[q, part(k)]).wait_send()


def schedule(K):
    seq = [("st0", 0), ("send", 0), ("st1", 0), ("send", 1), ("a", 0), ("st2", 0), ("send", 2), ("m1", 0), ("a", 1)]
    seq += [("send", k) for k in range(3, K)] + [("b1", 0)]
    for s in range(1, K + 4):
        for name, k in (
            ("m1", s), ("b2", s - 1), ("a", s + 1), ("b4", s - 2), ("b1", s), ("c2", s - 3), ("c1", s - 2),
            ("b3", s - 1), ("c3", s - 4),
        ):
            if 0 <= k < K:
                seq.append((name, k))
    return seq


def fused(tokens, norm_gain, hidden_bias, weight_in, weight_out, R, M, D, units):
    height, width = tokens.shape
    depth, ff = weight_in.shape
    half = ff // 2
    step = height // sum(units)
    cuts = [u * step for u in units]
    K = len(cuts)
    V = pltpu.VMEM
    S = pltpu.SemaphoreType.DMA
    vm = pl.BlockSpec(memory_space=pltpu.VMEM)
    hbm = pl.BlockSpec(memory_space=pltpu.HBM)
    return pl.pallas_call(
        functools.partial(kernel, R, M, D, cuts, schedule(K)),
        out_shape=jax.ShapeDtypeStruct(tokens.shape, BF16),
        in_specs=[vm, vm, vm, hbm, hbm],
        out_specs=vm,
        scratch_shapes=[
            V(weight_in.shape, BF16), V(weight_out.shape, BF16),
            V((2, R, height, width), BF16), V((2, R * max(cuts), width), BF16),
            V((M, 8, height), F32), V((R, 8, height), F32), V((R, height, 128), F32),
            V((2, R, height, half), BF16), V((2, 2, height, half), BF16), V((2, height, half), BF16),
            V((2, height, half), BF16), V((2, R, height, half), BF16),
            V((R, height, width), BF16), V((R, height, width), BF16), V((R, height, width), F32),
            V((R, height, width), BF16), V((R, height, width), BF16), V((R, height, width), BF16), S((2,)),
            S((K, R)), S((K, R)), S((K, R)), S((K, R)), S((M,)), S((M,)), S((3,)), S((R,)),
            S((K, 2, 2)), S((K, 2, 2)), S((K, 2)), S((K, 2)), S((K, 2, 3)), S((K, 2, R)), S((K,)), S((K,)),
            S((K, 3)), S((K, R)), S((K, R)), S((K, R)),
        ],
        compiler_params=pltpu.CompilerParams(
            collective_id=0, has_side_effects=True, vmem_limit_bytes=60 * 1024 * 1024
        ),
    )(tokens, norm_gain.reshape(M, 1, width), hidden_bias.reshape(1, ff), weight_in, weight_out)


def plain(tokens, norm_gain, hidden_bias, weight_in, weight_out, R, M, D):
    as_float = tokens.astype(F32)
    moment_sum, square_sum = lax.psum((jnp.sum(as_float, axis=1), jnp.sum(as_float * as_float, axis=1)), "mp")
    width = tokens.shape[1]
    gain = lax.dynamic_slice_in_dim(norm_gain, lax.axis_index("mp") * width, width)
    mean = moment_sum / D
    inverse = lax.rsqrt(jnp.maximum(square_sum / D - mean * mean, 0.0) + floor_value)
    part = ((as_float - mean[:, None]) * inverse[:, None] * gain[None, :]).astype(BF16)
    normed = lax.all_gather(part, "mp", axis=1, tiled=True)
    shuffled = lax.all_to_all(normed, "rows", split_axis=1, concat_axis=0, tiled=True)
    preact = lax.psum_scatter(
        jnp.dot(shuffled, weight_in, preferred_element_type=F32), "rows", scatter_dimension=0, tiled=True
    )
    hidden = jax.nn.gelu(preact + hidden_bias[None, :], approximate=False).astype(BF16)
    hidden = lax.all_gather(hidden, "rows", axis=0, tiled=True)
    terms = jnp.dot(hidden, weight_out, preferred_element_type=F32)
    terms = lax.all_to_all(terms, "rows", split_axis=0, concat_axis=1, tiled=True)
    branch = lax.psum_scatter(terms, "mp", scatter_dimension=1, tiled=True)
    return (as_float + branch).astype(BF16)


def solution(mesh):
    R, M = mesh.shape["rows"], mesh.shape["mp"]

    def body(tokens, norm_gain, hidden_bias, weight_in, weight_out):
        D = norm_gain.shape[0]
        aligned = tokens.shape[1] % 128 == 0 and weight_in.shape[1] % 512 == 0 and tokens.shape[0] == 16 * sum(UNITS)
        if R == 4 and M == 2 * R and aligned and tokens.shape[0] % 128 == 0:
            return fused(tokens, norm_gain, hidden_bias, weight_in, weight_out, R, M, D, UNITS)
        return plain(tokens, norm_gain, hidden_bias, weight_in, weight_out, R, M, D)

    return jax.shard_map(
        body,
        mesh=mesh,
        in_specs=(P("rows", "mp"), P(), P("mp"), P("rows", "mp"), P("mp", "rows")),
        out_specs=P("rows", "mp"),
        check_vma=False,
    )
```

```python
import functools

import jax
import jax.numpy as jnp
from jax import lax
from jax.experimental import pallas as pl
from jax.experimental.pallas import tpu as pltpu
from jax.sharding import PartitionSpec as P

MESH = pl.DeviceIdType.MESH
F32 = jnp.float32
BF16 = jnp.bfloat16
floor_value = 0.1
UNITS = (1, 2, 2, 2, 1)
FAR_IN = (2, 3, 4)
FAR_OUT = (0, 1)


def gelu(x):
    return 0.5 * x * (1.0 + lax.erf(x * 0.7071067811865476))


def kernel(
    R, M, D, cuts, order, far_in, far_out, tok, gain, bias, win_hbm, wout_hbm, out, win, wout, xs, nx, stc, mi, colst,
    pbuf, r1, r2, qbuf, hid, osend, osib, oown, csend, cmid, crecv, cfin, fin, wsem,
    s_a, s_ap, s_af, s_ax, r_a, r_af, s_sib, r_sib, s_st, r_st, s_mi, r_mi, s_b, s_f, r_p, r_q, r_g, r_ag,
    s_os, r_os, s_cm, s_cp, r_cm, s_cz, r_cz, s_fin, r_fin,
):
    r = lax.axis_index("rows")
    m = lax.axis_index("mp")
    Z = M // 2
    z, c = m // 2, m % 2
    sib = 2 * z + 1 - c
    height, width = tok.shape
    half = win.shape[1] // 2
    K = len(cuts)
    offs = [sum(cuts[:k]) for k in range(K)]
    rx, ry, rd = r + 1 - 2 * (r % 2), (r + 2) % 4, 3 - r
    first, second = (rx, ry), (ry, rx)
    peers = (rd, rx, ry)
    home = z == r

    pltpu.make_async_copy(win_hbm, win, wsem.at[0]).start()
    pltpu.make_async_copy(wout_hbm, wout, wsem.at[1]).start()

    def remote(src, dst, ssem, rsem, row, col):
        return pltpu.make_async_remote_copy(
            src_ref=src, dst_ref=dst, send_sem=ssem, recv_sem=rsem, device_id=(row, col), device_id_type=MESH
        )

    def part(k):
        return pl.ds(offs[k], cuts[k])

    def got(ref, sem):
        remote(ref, ref, sem, sem, r, sib).wait_recv()

    def sent(ref, sem):
        remote(ref, ref, sem, sem, r, sib).wait_send()

    barrier = pltpu.get_barrier_semaphore()

    def greet(row, col):
        pl.semaphore_signal(barrier, inc=1, device_id=(row, col), device_id_type=MESH)

    for i in range(1, M):
        greet(r, (m + i) % M)
    for i in range(1, R):
        greet((r + i) % R, m)

    @pl.when(jnp.logical_not(home))
    def _():
        for i in range(1, R):
            greet((r + i) % R, 2 * r + c)

    own = tok[...].astype(F32)
    lane = lax.broadcasted_iota(jnp.int32, (height, 128), 1)
    s1 = jnp.sum(own, axis=1, keepdims=True)
    s2 = jnp.sum(own * own, axis=1, keepdims=True)
    stc[m] = jnp.where(lane == 0, s1, s2).T[0:8]

    pl.semaphore_wait(barrier, (M - 1) + (R - 1) + jnp.where(home, 0, R - 1))

    toward = 2 * (z // 2) - 1

    def c_a(k, i):
        zd = (z + i * toward + Z) % Z
        return remote(tok.at[part(k)], xs.at[c, r, part(k)], (s_a if i else s_ap).at[0], r_a.at[k], z, 2 * zd + c)

    def c_sib(k, t, src):
        return remote(src, xs.at[c, t, part(k)], s_sib.at[0], r_sib.at[k], r, sib)

    def c_st(i):
        return remote(stc.at[m], stc.at[m], s_st.at[0], r_st.at[0], r, (m + i) % M)

    def c_mi(i):
        return remote(mi.at[r], mi.at[r], s_mi.at[0], r_mi.at[0], peers[i], m)

    def c_r1(k, h, i):
        tile = (first[h], rd)[i]
        return remote(
            pbuf.at[h, tile, part(k)], r1.at[h, i, part(k)], s_b.at[0], (r_q, r_p)[i].at[k, h], first[h], m
        )

    def c_r2(k, h):
        return remote(qbuf.at[h, part(k)], r2.at[h, part(k)], s_f.at[0], r_q.at[k, h], second[h], m)

    def c_ag(k, h, i):
        tile = (r, r, second[h])[i]
        to = (second[h], first[h], first[h])[i]
        ref = hid.at[h, tile, part(k)]
        return remote(ref, ref, (s_b, s_b, s_f)[i].at[0], r_g.at[k, h] if i == 0 else r_ag.at[k], to, m)

    def c_os(k):
        return remote(osend.at[:, part(k)], osib.at[:, part(k)], s_os.at[0], r_os.at[k], r, sib)

    def c_cm(k, i):
        t = peers[i]
        return remote(csend.at[t, part(k)], cmid.at[r, part(k)], s_cm.at[0], r_cm.at[k], t, m)

    def c_cz(k, q, src):
        return remote(src, crecv.at[z, part(k)], s_cz.at[0], r_cz.at[k], r, 2 * q + c)

    def plane_of(k, t):
        return (k + t) % Z

    def tile_of(k):
        return (z + Z * k - k) % Z

    def c_ax(k, i, src):
        t = tile_of(k)
        zd = (z + i * toward + Z) % Z
        return remote(src, xs.at[c, t, part(k)], s_ax.at[0], r_a.at[k], r, 2 * zd + c)

    def c_a1(k):
        return remote(
            tok.at[part(k)], xs.at[c, r, part(k)], s_af.at[far_in.index(k)], r_af.at[far_in.index(k)], z,
            2 * plane_of(k, r) + c,
        )

    def keeps(k):
        return home & (plane_of(k, r) == z)

    def c_cx(k, i):
        zd = (z + i * toward + Z) % Z
        t = (zd + Z * k - k) % Z
        return remote(csend.at[t, part(k)], crecv.at[z, part(k)], s_cz.at[0], r_cz.at[k], r, 2 * zd + c)

    def c_cp(k):
        return remote(cfin.at[part(k)], cmid.at[r, part(k)], s_cp.at[far_out.index(k)], r_cm.at[k], tile_of(k), m)

    def c_fin(k, q, src):
        j = far_out.index(k)
        return remote(src, fin.at[part(k)], s_fin.at[j], r_fin.at[j], r, 2 * q + c)

    def stage_send(k):
        if k in far_in:
            @pl.when(keeps(k))
            def _():
                xs[c, r, part(k)] = tok[part(k)]

            @pl.when(jnp.logical_not(keeps(k)))
            def _():
                c_a1(k).start()

            return
        for i in (1, 3, 2):
            c_a(k, i).start()

        @pl.when(home)
        def _():
            xs[c, r, part(k)] = tok[part(k)]
            c_sib(k, r, tok.at[part(k)]).start()

        @pl.when(jnp.logical_not(home))
        def _():
            c_a(k, 0).start()

    def stage_st0(_):
        for i in range(1, M):
            c_st(i).start()

    def stage_st1(_):
        got(stc.at[0:M - 1], r_st.at[0])
        tot = stc[0]
        for q in range(1, M):
            tot = tot + stc[q]
        mean = tot[0:1] / D
        var = jnp.maximum(tot[1:2] / D - mean * mean, 0.0)
        inv = lax.rsqrt(var + floor_value)
        sub = lax.broadcasted_iota(jnp.int32, (8, height), 0)
        mi[r] = jnp.where(sub == 0, mean, inv)
        for i in range(3):
            c_mi(i).start()

    def stage_st2(_):
        got(mi.at[0:R - 1], r_mi.at[0])
        sub = lax.broadcasted_iota(jnp.int32, (128, height), 0)
        for t in range(R):
            colst[t] = jnp.where(sub == 0, mi[t, 0:1], mi[t, 1:2]).T

    def stage_a1(k):
        if k not in far_in:
            return
        t = tile_of(k)

        def spread(src):
            for i in (1, 3, 2):
                c_ax(k, i, src).start()
            c_sib(k, t, src).start()

        @pl.when(keeps(k))
        def _():
            spread(tok.at[part(k)])

        @pl.when(jnp.logical_not(keeps(k)))
        def _():
            got(xs.at[c, t, part(k)], r_af.at[far_in.index(k)])
            spread(xs.at[c, t, part(k)])

    def stage_a(k):
        if k in far_in:
            got(xs.at[c, 0:R - 1, part(k)], r_a.at[k])
            for i in range(1, R):
                t = (tile_of(k) + i) % R
                c_sib(k, t, xs.at[c, t, part(k)]).start()
            return

        @pl.when(home)
        def _():
            got(xs.at[c, 0:R - 1, part(k)], r_a.at[k])

        @pl.when(jnp.logical_not(home))
        def _():
            got(xs.at[c, :, part(k)], r_a.at[k])
            c_sib(k, r, xs.at[c, r, part(k)]).start()

        for i in range(1, R):
            t = (r + i) % R
            c_sib(k, t, xs.at[c, t, part(k)]).start()

    def stage_m1(k):
        n = cuts[k]
        got(xs.at[1 - c, :, part(k)], r_sib.at[k])
        stats = colst[:, part(k)].reshape(R * n, 128)
        mean_c, inv_c = stats[:, 0:1], stats[:, 1:2]
        for cc in range(2):
            x = xs[cc, :, part(k)].astype(F32).reshape(R * n, width)
            nx[cc, 0:R * n] = ((x - mean_c) * inv_c * gain[2 * r + cc]).astype(BF16)

        if k == 0:
            pltpu.make_async_copy(win_hbm, win, wsem.at[0]).wait()

        tile = half // 2
        for h in range(2):
            def col(j, _):
                at = pl.multiple_of(j * tile, 128)
                wat = pl.multiple_of(h * half + j * tile, 128)
                acc = jnp.dot(nx[0, 0:R * n], win[0:width, pl.ds(wat, tile)], preferred_element_type=F32)
                acc += jnp.dot(nx[1, 0:R * n], win[width:2 * width, pl.ds(wat, tile)], preferred_element_type=F32)
                pbuf[h, :, part(k), pl.ds(at, tile)] = acc.astype(BF16).reshape(R, n, tile)
                return 0

            lax.fori_loop(0, 2, col, 0)
            c_r1(k, h, 1).start()
            c_r1(k, h, 0).start()

    def stage_b1(k):
        for h in range(2):
            got(r1.at[h, 1, part(k)], r_p.at[k, h])
            mine = pbuf[h, second[h], part(k)].astype(F32)
            qbuf[h, part(k)] = (mine + r1[h, 1, part(k)].astype(F32)).astype(BF16)
            c_r2(k, h).start()

    def stage_b2(k):
        for h in range(2):
            got(r1.at[h, :, part(k)], r_q.at[k, h])
            pre = pbuf[h, r, part(k)].astype(F32) + r1[h, 0, part(k)].astype(F32) + r2[h, part(k)].astype(F32)
            pre = pre + bias[0:1, h * half:(h + 1) * half]
            hid[h, r, part(k)] = gelu(pre).astype(BF16)
            c_ag(k, h, 0).start()
            c_ag(k, h, 1).start()

    def stage_b3(k):
        for h in range(2):
            got(hid.at[h, second[h], part(k)], r_g.at[k, h])
            c_ag(k, h, 2).start()

    def stage_b4(k):
        n = cuts[k]
        got(hid.at[:, 0:2, part(k)], r_ag.at[k])

        if k == 0:
            pltpu.make_async_copy(wout_hbm, wout, wsem.at[1]).wait()

        def product(cc):
            at = pl.multiple_of(cc * width, 128)
            acc = None
            for h in range(2):
                a = hid[h, :, part(k)].reshape(R * n, half)
                term = jnp.dot(a, wout[h * half:(h + 1) * half, pl.ds(at, width)], preferred_element_type=F32)
                acc = term if acc is None else acc + term
            return acc.reshape(R, n, width)

        osend[:, part(k)] = product(1 - c).astype(BF16)
        c_os(k).start()
        oown[:, part(k)] = product(c)

    def stage_c1(k):
        c_os(k).wait_recv()
        if k in far_out:
            t = tile_of(k)
            csend[:, part(k)] = (oown[:, part(k)] + osib[:, part(k)].astype(F32)).astype(BF16)
            for i in (1, 3, 2):
                c_cx(k, i).start()
            oown[t, part(k)] = oown[t, part(k)] + osib[t, part(k)].astype(F32)
            return
        csend[:, part(k)] = (oown[:, part(k)] + osib[:, part(k)].astype(F32)).astype(BF16)
        for i in range(3):
            c_cm(k, i).start()

        @pl.when(jnp.logical_not(home))
        def _():
            c_cz(k, r, csend.at[r, part(k)]).start()

    def stage_c2(k):
        if k in far_out:
            t = tile_of(k)
            total = oown[t, part(k)]
            got(crecv.at[0:Z - 1, part(k)], r_cz.at[k])
            for i in range(1, Z):
                q = (z + i) % Z
                total = total + crecv[q, part(k)].astype(F32)
            cfin[part(k)] = total.astype(BF16)

            @pl.when(t != r)
            def _():
                c_cp(k).start()

            return
        got(cmid.at[0:R - 1, part(k)], r_cm.at[k])
        for i in range(3):
            q = peers[i]

            @pl.when(q != z)
            def _():
                c_cz(k, q, cmid.at[q, part(k)]).start()

    def stage_c4(k):
        if k not in far_out:
            return

        @pl.when(tile_of(k) == r)
        def _():
            @pl.when(jnp.logical_not(home))
            def _():
                c_fin(k, r, cfin.at[part(k)]).start()

            got(cmid.at[0:R - 1, part(k)], r_cm.at[k])
            for i in range(3):
                q = peers[i]

                @pl.when(q != z)
                def _():
                    c_fin(k, q, cmid.at[q, part(k)]).start()

    def stage_c3(k):
        if k in far_out:
            mine = tile_of(k) == r

            @pl.when(mine & home)
            def _():
                fin[part(k)] = cfin[part(k)]

            @pl.when(mine & jnp.logical_not(home))
            def _():
                fin[part(k)] = cmid[z, part(k)]

            @pl.when(jnp.logical_not(mine))
            def _():
                got(fin.at[part(k)], r_fin.at[far_out.index(k)])

            out[part(k)] = (tok[part(k)].astype(F32) + fin[part(k)].astype(F32)).astype(BF16)
            return

        @pl.when(home)
        def _():
            crecv[z, part(k)] = csend[r, part(k)]

        @pl.when(jnp.logical_not(home))
        def _():
            crecv[z, part(k)] = cmid[z, part(k)]

        got(crecv.at[0:Z - 1, part(k)], r_cz.at[k])
        total = (crecv[0, part(k)].astype(F32) + crecv[1, part(k)].astype(F32)) + (
            crecv[2, part(k)].astype(F32) + crecv[3, part(k)].astype(F32)
        )
        out[part(k)] = (tok[part(k)].astype(F32) + total).astype(BF16)

    def stage_e(_):
        near = sum(cuts[k] for k in range(K) if k not in far_in)
        sent(xs.at[0, 0:Z - 1, 0:near], s_a.at[0])
        sent(xs.at[0, 0:Z - 1, near:height], s_ax.at[0])

        @pl.when(jnp.logical_not(home))
        def _():
            sent(tok.at[0:near], s_ap.at[0])

        for k in far_in:
            @pl.when(jnp.logical_not(keeps(k)))
            def _():
                c_a1(k).wait_send()

        sent(xs.at[0], s_sib.at[0])
        sent(stc.at[0:M - 1], s_st.at[0])
        sent(mi.at[0:R - 1], s_mi.at[0])
        sent(hid, s_b.at[0])
        sent(hid.at[:, 0:2], s_f.at[0])
        sent(osend, s_os.at[0])
        sent(csend.at[0:R - 1, 0:sum(cuts[k] for k in range(K) if k not in far_out)], s_cm.at[0])
        for k in far_out:
            @pl.when(tile_of(k) != r)
            def _():
                c_cp(k).wait_send()

            @pl.when(tile_of(k) == r)
            def _():
                sent(crecv.at[0:Z - 1, part(k)], s_fin.at[far_out.index(k)])

        sent(crecv.at[0:Z - 1], s_cz.at[0])

    stages = {
        "send": stage_send, "st0": stage_st0, "st1": stage_st1, "st2": stage_st2, "a1": stage_a1, "a": stage_a,
        "m1": stage_m1, "b1": stage_b1, "b2": stage_b2, "b3": stage_b3, "b4": stage_b4, "c1": stage_c1,
        "c2": stage_c2, "c4": stage_c4, "c3": stage_c3, "e": stage_e,
    }
    assert len(set(order)) == len(order)
    for name, k in order:
        stages[name](k)


ORDER = (
    "st0_0 send_0 send_1",
    "send_2 send_3 send_4",
    "st1_0 a_0 st2_0",
    "m1_0 a_1 m1_1",
    "a1_2 b1_0 a1_3",
    "b1_1 b2_0 a_2",
    "b2_1 a1_4 m1_2",
    "b3_0 a_3 b3_1",
    "b1_2 a_4 m1_3",
    "b4_0 m1_4 b1_3",
    "b4_1 b2_2 c1_1",
    "b2_3 c1_0 b1_4",
    "b3_2 c2_1 b3_3",
    "c2_0 b2_4 b4_2",
    "c1_2 b4_3 c4_1",
    "b3_4 c1_3 c4_0",
    "c2_2 b4_4 c1_4",
    "c3_0 c2_3 c2_4",
    "c3_1 c3_2 c3_3",
    "c3_4 e_0",
)


def schedule(K):
    names = " ".join(ORDER).split()
    return [(name.split("_")[0], int(name.split("_")[1])) for name in names]


def fused(tokens, norm_gain, hidden_bias, weight_in, weight_out, R, M, D, units):
    height, width = tokens.shape
    depth, ff = weight_in.shape
    half = ff // 2
    step = height // sum(units)
    cuts = [u * step for u in units]
    K = len(cuts)
    V = pltpu.VMEM
    S = pltpu.SemaphoreType.DMA
    vm = pl.BlockSpec(memory_space=pltpu.VMEM)
    hbm = pl.BlockSpec(memory_space=pltpu.HBM)
    return pl.pallas_call(
        functools.partial(kernel, R, M, D, cuts, schedule(K), FAR_IN, FAR_OUT),
        out_shape=jax.ShapeDtypeStruct(tokens.shape, BF16),
        in_specs=[vm, vm, vm, hbm, hbm],
        out_specs=vm,
        scratch_shapes=[
            V(weight_in.shape, BF16), V(weight_out.shape, BF16),
            V((2, R, height, width), BF16), V((2, R * max(cuts), width), BF16),
            V((M, 8, height), F32), V((R, 8, height), F32), V((R, height, 128), F32),
            V((2, R, height, half), BF16), V((2, 2, height, half), BF16), V((2, height, half), BF16),
            V((2, height, half), BF16), V((2, R, height, half), BF16),
            V((R, height, width), BF16), V((R, height, width), BF16), V((R, height, width), F32),
            V((R, height, width), BF16), V((R, height, width), BF16), V((R, height, width), BF16),
            V((height, width), BF16), V((height, width), BF16), S((2,)),
            S((1,)), S((1,)), S((len(FAR_IN),)), S((1,)), S((K,)), S((len(FAR_IN),)), S((1,)), S((K,)), S((1,)), S((1,)),
            S((1,)), S((1,)), S((1,)), S((1,)), S((K, 2)), S((K, 2)), S((K, 2)), S((K,)),
            S((1,)), S((K,)), S((1,)), S((len(FAR_OUT),)), S((K,)), S((1,)), S((K,)), S((len(FAR_OUT),)), S((len(FAR_OUT),)),
        ],
        compiler_params=pltpu.CompilerParams(
            collective_id=0, has_side_effects=True, vmem_limit_bytes=60 * 1024 * 1024
        ),
    )(tokens, norm_gain.reshape(M, 1, width), hidden_bias.reshape(1, ff), weight_in, weight_out)


def plain(tokens, norm_gain, hidden_bias, weight_in, weight_out, R, M, D):
    as_float = tokens.astype(F32)
    moment_sum, square_sum = lax.psum((jnp.sum(as_float, axis=1), jnp.sum(as_float * as_float, axis=1)), "mp")
    width = tokens.shape[1]
    gain = lax.dynamic_slice_in_dim(norm_gain, lax.axis_index("mp") * width, width)
    mean = moment_sum / D
    inverse = lax.rsqrt(jnp.maximum(square_sum / D - mean * mean, 0.0) + floor_value)
    part = ((as_float - mean[:, None]) * inverse[:, None] * gain[None, :]).astype(BF16)
    normed = lax.all_gather(part, "mp", axis=1, tiled=True)
    shuffled = lax.all_to_all(normed, "rows", split_axis=1, concat_axis=0, tiled=True)
    preact = lax.psum_scatter(
        jnp.dot(shuffled, weight_in, preferred_element_type=F32), "rows", scatter_dimension=0, tiled=True
    )
    hidden = jax.nn.gelu(preact + hidden_bias[None, :], approximate=False).astype(BF16)
    hidden = lax.all_gather(hidden, "rows", axis=0, tiled=True)
    terms = jnp.dot(hidden, weight_out, preferred_element_type=F32)
    terms = lax.all_to_all(terms, "rows", split_axis=0, concat_axis=1, tiled=True)
    branch = lax.psum_scatter(terms, "mp", scatter_dimension=1, tiled=True)
    return (as_float + branch).astype(BF16)


def solution(mesh):
    R, M = mesh.shape["rows"], mesh.shape["mp"]

    def body(tokens, norm_gain, hidden_bias, weight_in, weight_out):
        D = norm_gain.shape[0]
        aligned = tokens.shape[1] % 128 == 0 and weight_in.shape[1] % 512 == 0 and tokens.shape[0] == 16 * sum(UNITS)
        if R == 4 and M == 2 * R and aligned and tokens.shape[0] % 128 == 0:
            return fused(tokens, norm_gain, hidden_bias, weight_in, weight_out, R, M, D, UNITS)
        return plain(tokens, norm_gain, hidden_bias, weight_in, weight_out, R, M, D)

    return jax.shard_map(
        body,
        mesh=mesh,
        in_specs=(P("rows", "mp"), P(), P("mp"), P("rows", "mp"), P("mp", "rows")),
        out_specs=P("rows", "mp"),
        check_vma=False,
    )
```

```python
import functools

import jax
import jax.numpy as jnp
from jax import lax
from jax.experimental import pallas as pl
from jax.experimental.pallas import tpu as pltpu
from jax.sharding import PartitionSpec as P

MESH = pl.DeviceIdType.MESH
F32 = jnp.float32
BF16 = jnp.bfloat16
floor_value = 0.1
UNITS = ((1,), (2,), (2,), (1,), (1,), (1,))
FAR_IN = (2, 3, 4, 5)
FAR_OUT = (0, 1, 2, 3)


def gelu(x):
    return 0.5 * x * (1.0 + lax.erf(x * 0.7071067811865476))


def kernel(
    R, M, D, groups, order, far_in, far_out, tok_hbm, gain_hbm, bias_hbm, win_hbm, wout_hbm, out, tok, gain, bias,
    win, wout, xs, nx, stc, mi, colst,
    pbuf, r1, r2, qbuf, hid, osend, osib, oown, csend, cmid, crecv, cfin, fin, wsem,
    s_a, s_ap, s_af, s_ax, r_a, r_af, s_sib, r_sib, s_st, r_st, s_mi, r_mi, s_b, s_f, r_p, r_q, r_g, r_ag,
    s_os, r_os, s_cm, s_cp, r_cm, s_cz, r_cz, s_fin, r_fin,
):
    r = lax.axis_index("rows")
    m = lax.axis_index("mp")
    Z = M // 2
    z, c = m // 2, m % 2
    sib = 2 * z + 1 - c
    height, width = tok.shape
    cuts = [n for group in groups for n in group]
    wide = [sum(group) for group in groups]
    firsts = [sum(len(group) for group in groups[:g]) for g in range(len(groups))]
    subs = [range(firsts[g], firsts[g] + len(groups[g])) for g in range(len(groups))]
    G = len(groups)
    half = win.shape[1] // 2
    K = len(cuts)
    offs = [sum(cuts[:k]) for k in range(K)]
    rx, ry, rd = r + 1 - 2 * (r % 2), (r + 2) % 4, 3 - r
    first, second = (rx, ry), (ry, rx)
    peers = (rd, rx, ry)
    home = z == r

    in_tok = pltpu.make_async_copy(tok_hbm, tok, wsem.at[2])
    in_gain = pltpu.make_async_copy(gain_hbm, gain, wsem.at[3])
    in_bias = pltpu.make_async_copy(bias_hbm, bias, wsem.at[4])
    in_tok.start()

    def remote(src, dst, ssem, rsem, row, col):
        return pltpu.make_async_remote_copy(
            src_ref=src, dst_ref=dst, send_sem=ssem, recv_sem=rsem, device_id=(row, col), device_id_type=MESH
        )

    def part(k):
        return pl.ds(offs[k], cuts[k])

    def span(g):
        return pl.ds(offs[firsts[g]], wide[g])

    def got(ref, sem):
        remote(ref, ref, sem, sem, r, sib).wait_recv()

    def sent(ref, sem):
        remote(ref, ref, sem, sem, r, sib).wait_send()

    barrier = pltpu.get_barrier_semaphore()

    def greet(row, col):
        pl.semaphore_signal(barrier, inc=1, device_id=(row, col), device_id_type=MESH)

    for i in range(1, M):
        greet(r, (m + i) % M)
    for i in range(1, R):
        greet((r + i) % R, m)

    @pl.when(jnp.logical_not(home))
    def _():
        for i in range(1, R):
            greet((r + i) % R, 2 * r + c)

    in_gain.start()
    in_bias.start()
    pltpu.make_async_copy(win_hbm, win, wsem.at[0]).start()
    pltpu.make_async_copy(wout_hbm, wout, wsem.at[1]).start()
    in_tok.wait()
    own = tok[...].astype(F32)
    lane = lax.broadcasted_iota(jnp.int32, (height, 128), 1)
    s1 = jnp.sum(own, axis=1, keepdims=True)
    s2 = jnp.sum(own * own, axis=1, keepdims=True)
    stc[m] = jnp.where(lane == 0, s1, s2).T[0:8]

    pl.semaphore_wait(barrier, (M - 1) + (R - 1) + jnp.where(home, 0, R - 1))

    toward = 2 * (z // 2) - 1

    def c_a(k, i):
        zd = (z + i * toward + Z) % Z
        return remote(tok.at[span(k)], xs.at[c, r, span(k)], (s_a if i else s_ap).at[0], r_a.at[k], z, 2 * zd + c)

    def c_sib(k, t, src):
        return remote(src, xs.at[c, t, span(k)], s_sib.at[0], r_sib.at[k], r, sib)

    def c_st(i):
        return remote(stc.at[m], stc.at[m], s_st.at[0], r_st.at[0], r, (m + i) % M)

    def c_mi(i):
        return remote(mi.at[r], mi.at[r], s_mi.at[0], r_mi.at[0], peers[i], m)

    def c_r1(k, h, i):
        tile = (first[h], rd)[i]
        return remote(
            pbuf.at[h, tile, part(k)], r1.at[h, i, part(k)], s_b.at[0], (r_q, r_p)[i].at[k, h], first[h], m
        )

    def c_r2(k, h):
        return remote(qbuf.at[h, part(k)], r2.at[h, part(k)], s_f.at[0], r_q.at[k, h], second[h], m)

    def c_ag(k, h, i):
        tile = (r, r, second[h])[i]
        to = (second[h], first[h], first[h])[i]
        ref = hid.at[h, tile, part(k)]
        return remote(ref, ref, (s_b, s_b, s_f)[i].at[0], r_g.at[k, h] if i == 0 else r_ag.at[k], to, m)

    def c_os(k):
        return remote(osend.at[:, span(k)], osib.at[:, span(k)], s_os.at[0], r_os.at[k], r, sib)

    def c_cm(k, i):
        t = peers[i]
        return remote(csend.at[t, span(k)], cmid.at[r, span(k)], s_cm.at[0], r_cm.at[k], t, m)

    def c_cz(k, q, src):
        return remote(src, crecv.at[z, span(k)], s_cz.at[0], r_cz.at[k], r, 2 * q + c)

    def plane_of(k, t):
        return (k + t) % Z

    def tile_of(k):
        return (z + Z * k - k) % Z

    def c_ax(k, i, src):
        t = tile_of(k)
        zd = (z + i * toward + Z) % Z
        return remote(src, xs.at[c, t, span(k)], s_ax.at[0], r_a.at[k], r, 2 * zd + c)

    def c_a1(k):
        return remote(
            tok.at[span(k)], xs.at[c, r, span(k)], s_af.at[far_in.index(k)], r_af.at[far_in.index(k)], z,
            2 * plane_of(k, r) + c,
        )

    def keeps(k):
        return home & (plane_of(k, r) == z)

    def c_cx(k, i):
        zd = (z + i * toward + Z) % Z
        t = (zd + Z * k - k) % Z
        return remote(csend.at[t, span(k)], crecv.at[z, span(k)], s_cz.at[0], r_cz.at[k], r, 2 * zd + c)

    def c_cp(k):
        return remote(cfin.at[span(k)], cmid.at[r, span(k)], s_cp.at[far_out.index(k)], r_cm.at[k], tile_of(k), m)

    def c_fin(k, q, src):
        j = far_out.index(k)
        return remote(src, fin.at[span(k)], s_fin.at[j], r_fin.at[j], r, 2 * q + c)

    def stage_send(k):
        if k in far_in:
            @pl.when(keeps(k))
            def _():
                xs[c, r, span(k)] = tok[span(k)]

            @pl.when(jnp.logical_not(keeps(k)))
            def _():
                c_a1(k).start()

            return
        for i in (1, 3, 2):
            c_a(k, i).start()

        @pl.when(home)
        def _():
            xs[c, r, span(k)] = tok[span(k)]
            c_sib(k, r, tok.at[span(k)]).start()

        @pl.when(jnp.logical_not(home))
        def _():
            c_a(k, 0).start()

    def stage_st0(_):
        for i in range(1, M):
            c_st(i).start()

    def stage_st1(_):
        got(stc.at[0:M - 1], r_st.at[0])
        tot = stc[0]
        for q in range(1, M):
            tot = tot + stc[q]
        mean = tot[0:1] / D
        var = jnp.maximum(tot[1:2] / D - mean * mean, 0.0)
        inv = lax.rsqrt(var + floor_value)
        sub = lax.broadcasted_iota(jnp.int32, (8, height), 0)
        mi[r] = jnp.where(sub == 0, mean, inv)
        for i in range(3):
            c_mi(i).start()

    def stage_st2(_):
        got(mi.at[0:R - 1], r_mi.at[0])
        sub = lax.broadcasted_iota(jnp.int32, (128, height), 0)
        for t in range(R):
            colst[t] = jnp.where(sub == 0, mi[t, 0:1], mi[t, 1:2]).T

    def stage_a1(k):
        if k not in far_in:
            return
        t = tile_of(k)

        def spread(src):
            for i in (1, 3, 2):
                c_ax(k, i, src).start()
            c_sib(k, t, src).start()

        @pl.when(keeps(k))
        def _():
            spread(tok.at[span(k)])

        @pl.when(jnp.logical_not(keeps(k)))
        def _():
            got(xs.at[c, t, span(k)], r_af.at[far_in.index(k)])
            spread(xs.at[c, t, span(k)])

    def stage_a(k):
        if k in far_in:
            got(xs.at[c, 0:R - 1, span(k)], r_a.at[k])
            for i in range(1, R):
                t = (tile_of(k) + i) % R
                c_sib(k, t, xs.at[c, t, span(k)]).start()
            return

        @pl.when(home)
        def _():
            got(xs.at[c, 0:R - 1, span(k)], r_a.at[k])

        @pl.when(jnp.logical_not(home))
        def _():
            got(xs.at[c, :, span(k)], r_a.at[k])
            c_sib(k, r, xs.at[c, r, span(k)]).start()

        for i in range(1, R):
            t = (r + i) % R
            c_sib(k, t, xs.at[c, t, span(k)]).start()

    def stage_m1(k):
        n = wide[k]
        got(xs.at[1 - c, :, span(k)], r_sib.at[k])
        if k == 0:
            in_gain.wait()
        stats = colst[:, span(k)].reshape(R * n, 128)
        mean_c, inv_c = stats[:, 0:1], stats[:, 1:2]
        for cc in range(2):
            x = xs[cc, :, span(k)].astype(F32).reshape(R * n, width)
            nx[cc, 0:R * n] = ((x - mean_c) * inv_c * gain[2 * r + cc]).astype(BF16)

        if k == 0:
            pltpu.make_async_copy(win_hbm, win, wsem.at[0]).wait()
            in_bias.wait()

        tile = half // 2
        for h in range(2):
            def col(j, _):
                at = pl.multiple_of(j * tile, 128)
                wat = pl.multiple_of(h * half + j * tile, 128)
                acc = jnp.dot(nx[0, 0:R * n], win[0:width, pl.ds(wat, tile)], preferred_element_type=F32)
                acc += jnp.dot(nx[1, 0:R * n], win[width:2 * width, pl.ds(wat, tile)], preferred_element_type=F32)
                pbuf[h, :, span(k), pl.ds(at, tile)] = acc.astype(BF16).reshape(R, n, tile)
                return 0

            lax.fori_loop(0, 2, col, 0)
            for sub in subs[k]:
                c_r1(sub, h, 1).start()
                c_r1(sub, h, 0).start()

    def stage_b1(k):
        for h in range(2):
            got(r1.at[h, 1, part(k)], r_p.at[k, h])
            mine = pbuf[h, second[h], part(k)].astype(F32)
            qbuf[h, part(k)] = (mine + r1[h, 1, part(k)].astype(F32)).astype(BF16)
            c_r2(k, h).start()

    def stage_b2(k):
        for h in range(2):
            got(r1.at[h, :, part(k)], r_q.at[k, h])
            pre = pbuf[h, r, part(k)].astype(F32) + r1[h, 0, part(k)].astype(F32) + r2[h, part(k)].astype(F32)
            pre = pre + bias[0:1, h * half:(h + 1) * half]
            hid[h, r, part(k)] = gelu(pre).astype(BF16)
            c_ag(k, h, 0).start()
            c_ag(k, h, 1).start()

    def stage_b3(k):
        for h in range(2):
            got(hid.at[h, second[h], part(k)], r_g.at[k, h])
            c_ag(k, h, 2).start()

    def stage_b4(k):
        n = wide[k]
        for sub in subs[k]:
            got(hid.at[:, 0:2, part(sub)], r_ag.at[sub])

        if k == 0:
            pltpu.make_async_copy(wout_hbm, wout, wsem.at[1]).wait()

        def product(cc):
            at = pl.multiple_of(cc * width, 128)
            acc = None
            for h in range(2):
                a = hid[h, :, span(k)].reshape(R * n, half)
                term = jnp.dot(a, wout[h * half:(h + 1) * half, pl.ds(at, width)], preferred_element_type=F32)
                acc = term if acc is None else acc + term
            return acc.reshape(R, n, width)

        osend[:, span(k)] = product(1 - c).astype(BF16)
        c_os(k).start()
        oown[:, span(k)] = product(c)

    def stage_c1(k):
        c_os(k).wait_recv()
        if k in far_out:
            t = tile_of(k)
            csend[:, span(k)] = (oown[:, span(k)] + osib[:, span(k)].astype(F32)).astype(BF16)
            for i in (1, 3, 2):
                c_cx(k, i).start()
            oown[t, span(k)] = oown[t, span(k)] + osib[t, span(k)].astype(F32)
            return
        csend[:, span(k)] = (oown[:, span(k)] + osib[:, span(k)].astype(F32)).astype(BF16)
        for i in range(3):
            c_cm(k, i).start()

        @pl.when(jnp.logical_not(home))
        def _():
            c_cz(k, r, csend.at[r, span(k)]).start()

    def stage_c2(k):
        if k in far_out:
            t = tile_of(k)
            total = oown[t, span(k)]
            got(crecv.at[0:Z - 1, span(k)], r_cz.at[k])
            for i in range(1, Z):
                q = (z + i) % Z
                total = total + crecv[q, span(k)].astype(F32)
            cfin[span(k)] = total.astype(BF16)

            @pl.when(t != r)
            def _():
                c_cp(k).start()

            return
        got(cmid.at[0:R - 1, span(k)], r_cm.at[k])
        for i in range(3):
            q = peers[i]

            @pl.when(q != z)
            def _():
                c_cz(k, q, cmid.at[q, span(k)]).start()

    def stage_c4(k):
        if k not in far_out:
            return

        @pl.when(tile_of(k) == r)
        def _():
            @pl.when(jnp.logical_not(home))
            def _():
                c_fin(k, r, cfin.at[span(k)]).start()

            got(cmid.at[0:R - 1, span(k)], r_cm.at[k])
            for i in range(3):
                q = peers[i]

                @pl.when(q != z)
                def _():
                    c_fin(k, q, cmid.at[q, span(k)]).start()

    def stage_c3(k):
        if k in far_out:
            mine = tile_of(k) == r

            @pl.when(mine & home)
            def _():
                fin[span(k)] = cfin[span(k)]

            @pl.when(mine & jnp.logical_not(home))
            def _():
                fin[span(k)] = cmid[z, span(k)]

            @pl.when(jnp.logical_not(mine))
            def _():
                got(fin.at[span(k)], r_fin.at[far_out.index(k)])

            out[span(k)] = (tok[span(k)].astype(F32) + fin[span(k)].astype(F32)).astype(BF16)
            return

        @pl.when(home)
        def _():
            crecv[z, span(k)] = csend[r, span(k)]

        @pl.when(jnp.logical_not(home))
        def _():
            crecv[z, span(k)] = cmid[z, span(k)]

        got(crecv.at[0:Z - 1, span(k)], r_cz.at[k])
        total = (crecv[0, span(k)].astype(F32) + crecv[1, span(k)].astype(F32)) + (
            crecv[2, span(k)].astype(F32) + crecv[3, span(k)].astype(F32)
        )
        out[span(k)] = (tok[span(k)].astype(F32) + total).astype(BF16)

    def stage_e(_):
        near = sum(wide[k] for k in range(G) if k not in far_in)
        sent(xs.at[0, 0:Z - 1, 0:near], s_a.at[0])
        sent(xs.at[0, 0:Z - 1, near:height], s_ax.at[0])

        @pl.when(jnp.logical_not(home))
        def _():
            sent(tok.at[0:near], s_ap.at[0])

        for k in far_in:
            @pl.when(jnp.logical_not(keeps(k)))
            def _():
                c_a1(k).wait_send()

        sent(xs.at[0], s_sib.at[0])
        sent(stc.at[0:M - 1], s_st.at[0])
        sent(mi.at[0:R - 1], s_mi.at[0])
        sent(hid, s_b.at[0])
        sent(hid.at[:, 0:2], s_f.at[0])
        sent(osend, s_os.at[0])
        sent(csend.at[0:R - 1, 0:sum(wide[k] for k in range(G) if k not in far_out)], s_cm.at[0])
        for k in far_out:
            @pl.when(tile_of(k) != r)
            def _():
                c_cp(k).wait_send()

            @pl.when(tile_of(k) == r)
            def _():
                sent(crecv.at[0:Z - 1, span(k)], s_fin.at[far_out.index(k)])

        sent(crecv.at[0:Z - 1], s_cz.at[0])

    stages = {
        "send": stage_send, "st0": stage_st0, "st1": stage_st1, "st2": stage_st2, "a1": stage_a1, "a": stage_a,
        "m1": stage_m1, "b1": stage_b1, "b2": stage_b2, "b3": stage_b3, "b4": stage_b4, "c1": stage_c1,
        "c2": stage_c2, "c4": stage_c4, "c3": stage_c3, "e": stage_e,
    }
    assert len(set(order)) == len(order)
    for name, k in order:
        stages[name](k)


ORDER = (
    "st0_0 send_0 send_1",
    "send_2 send_3 send_4",
    "send_5 st1_0 a_0",
    "st2_0 m1_0 a_1",
    "m1_1 b1_0 a1_2",
    "a1_5 b1_1 b2_0",
    "b2_1 a1_4 a_2",
    "a1_3 m1_2 b3_0",
    "b1_2 a_3 b3_1",
    "m1_3 b2_2 a_4",
    "b4_0 b1_3 m1_4",
    "b4_1 c1_1 c1_0",
    "b3_2 a_5 b2_3",
    "m1_5 b1_4 b4_2",
    "b3_3 c1_2 b1_5",
    "b2_4 b2_5 b4_3",
    "b3_4 c2_1 c1_3",
    "c2_0 c2_2 b3_5",
    "b4_4 c1_4 c2_3",
    "c4_0 c4_1 b4_5",
    "c4_2 c1_5 c2_4",
    "c4_3 c2_5 c3_0",
    "c3_3 c3_2 c3_4",
    "c3_1 c3_5 e_0",
)


def schedule():
    names = " ".join(ORDER).split()
    return [(name.split("_")[0], int(name.split("_")[1])) for name in names]


def fused(tokens, norm_gain, hidden_bias, weight_in, weight_out, R, M, D):
    height, width = tokens.shape
    depth, ff = weight_in.shape
    half = ff // 2
    step = height // sum(sum(group) for group in UNITS)
    groups = [[u * step for u in group] for group in UNITS]
    K, G = sum(len(group) for group in groups), len(groups)
    V = pltpu.VMEM
    S = pltpu.SemaphoreType.DMA
    vm = pl.BlockSpec(memory_space=pltpu.VMEM)
    hbm = pl.BlockSpec(memory_space=pltpu.HBM)
    return pl.pallas_call(
        functools.partial(kernel, R, M, D, groups, schedule(), FAR_IN, FAR_OUT),
        out_shape=pltpu.VMEM(tokens.shape, BF16),
        in_specs=[hbm, hbm, hbm, hbm, hbm],
        out_specs=vm,
        scratch_shapes=[
            V(tokens.shape, BF16), V((M, 1, width), F32), V((1, ff), F32), V(weight_in.shape, BF16), V(weight_out.shape, BF16),
            V((2, R, height, width), BF16), V((2, R * max(sum(group) for group in groups), width), BF16),
            V((M, 8, height), F32), V((R, 8, height), F32), V((R, height, 128), F32),
            V((2, R, height, half), BF16), V((2, 2, height, half), BF16), V((2, height, half), BF16),
            V((2, height, half), BF16), V((2, R, height, half), BF16),
            V((R, height, width), BF16), V((R, height, width), BF16), V((R, height, width), F32),
            V((R, height, width), BF16), V((R, height, width), BF16), V((R, height, width), BF16),
            V((height, width), BF16), V((height, width), BF16), S((5,)),
            S((1,)), S((1,)), S((len(FAR_IN),)), S((1,)), S((G,)), S((len(FAR_IN),)), S((1,)), S((G,)), S((1,)), S((1,)),
            S((1,)), S((1,)), S((1,)), S((1,)), S((K, 2)), S((K, 2)), S((K, 2)), S((K,)),
            S((1,)), S((G,)), S((1,)), S((len(FAR_OUT),)), S((G,)), S((1,)), S((G,)), S((len(FAR_OUT),)), S((len(FAR_OUT),)),
        ],
        compiler_params=pltpu.CompilerParams(
            collective_id=0, has_side_effects=True, vmem_limit_bytes=60 * 1024 * 1024
        ),
    )(tokens, norm_gain.reshape(M, 1, width), hidden_bias.reshape(1, ff), weight_in, weight_out)


def plain(tokens, norm_gain, hidden_bias, weight_in, weight_out, R, M, D):
    as_float = tokens.astype(F32)
    moment_sum, square_sum = lax.psum((jnp.sum(as_float, axis=1), jnp.sum(as_float * as_float, axis=1)), "mp")
    width = tokens.shape[1]
    gain = lax.dynamic_slice_in_dim(norm_gain, lax.axis_index("mp") * width, width)
    mean = moment_sum / D
    inverse = lax.rsqrt(jnp.maximum(square_sum / D - mean * mean, 0.0) + floor_value)
    part = ((as_float - mean[:, None]) * inverse[:, None] * gain[None, :]).astype(BF16)
    normed = lax.all_gather(part, "mp", axis=1, tiled=True)
    shuffled = lax.all_to_all(normed, "rows", split_axis=1, concat_axis=0, tiled=True)
    preact = lax.psum_scatter(
        jnp.dot(shuffled, weight_in, preferred_element_type=F32), "rows", scatter_dimension=0, tiled=True
    )
    hidden = jax.nn.gelu(preact + hidden_bias[None, :], approximate=False).astype(BF16)
    hidden = lax.all_gather(hidden, "rows", axis=0, tiled=True)
    terms = jnp.dot(hidden, weight_out, preferred_element_type=F32)
    terms = lax.all_to_all(terms, "rows", split_axis=0, concat_axis=1, tiled=True)
    branch = lax.psum_scatter(terms, "mp", scatter_dimension=1, tiled=True)
    return (as_float + branch).astype(BF16)


def solution(mesh):
    R, M = mesh.shape["rows"], mesh.shape["mp"]

    def body(tokens, norm_gain, hidden_bias, weight_in, weight_out):
        D = norm_gain.shape[0]
        aligned = tokens.shape[1] % 128 == 0 and weight_in.shape[1] % 512 == 0 and tokens.shape[0] == 16 * sum(sum(group) for group in UNITS)
        if R == 4 and M == 2 * R and aligned and tokens.shape[0] % 128 == 0:
            return fused(tokens, norm_gain, hidden_bias, weight_in, weight_out, R, M, D)
        return plain(tokens, norm_gain, hidden_bias, weight_in, weight_out, R, M, D)

    return jax.shard_map(
        body,
        mesh=mesh,
        in_specs=(P("rows", "mp"), P(), P("mp"), P("rows", "mp"), P("mp", "rows")),
        out_specs=P("rows", "mp"),
        check_vma=False,
    )
```

```python
import functools

import jax
import jax.numpy as jnp
from jax import lax
from jax.experimental import pallas as pl
from jax.experimental.pallas import tpu as pltpu
from jax.sharding import PartitionSpec as P

MESH = pl.DeviceIdType.MESH
F32 = jnp.float32
BF16 = jnp.bfloat16
floor_value = 0.1
SPLIT = 2
UNITS = ((1,), (2,), (2,), (1,), (1,), (1,))
FAR_IN = (2, 3, 4, 5)
FAR_OUT = (0, 1, 2, 3)


def gelu(x):
    return 0.5 * x * (1.0 + lax.erf(x * 0.7071067811865476))


def kernel(
    R, M, D, groups, order, far_in, far_out, tok_hbm, gain_hbm, bias_hbm, win_hbm, wout_hbm, out, tok, gain, bias,
    win, wout, xs, nx, stc, mi, colst,
    pbuf, r1, r2, qbuf, hid, osend, osib, oown, csend, cmid, crecv, cfin, fin, wsem,
    s_a, s_ap, s_af, s_ax, r_a, r_af, s_sib, r_sib, s_st, r_st, s_mi, r_mi, s_b, s_f, r_p, r_q, r_g, r_ag,
    s_os, r_os, s_cm, s_cp, r_cm, s_cz, r_cz, s_fin, r_fin,
):
    r = lax.axis_index("rows")
    m = lax.axis_index("mp")
    Z = M // 2
    z, c = m // 2, m % 2
    sib = 2 * z + 1 - c
    height, width = tok.shape
    cuts = [n for group in groups for n in group]
    wide = [sum(group) for group in groups]
    firsts = [sum(len(group) for group in groups[:g]) for g in range(len(groups))]
    subs = [range(firsts[g], firsts[g] + len(groups[g])) for g in range(len(groups))]
    G = len(groups)
    half = win.shape[1] // 2
    K = len(cuts)
    offs = [sum(cuts[:k]) for k in range(K)]
    rx, ry, rd = r + 1 - 2 * (r % 2), (r + 2) % 4, 3 - r
    first, second = (rx, ry), (ry, rx)
    peers = (rd, rx, ry)
    home = z == r

    in_tok = pltpu.make_async_copy(tok_hbm, tok, wsem.at[2])
    in_gain = pltpu.make_async_copy(gain_hbm, gain, wsem.at[3])
    in_bias = pltpu.make_async_copy(bias_hbm, bias, wsem.at[4])
    in_tok.start()

    def remote(src, dst, ssem, rsem, row, col):
        return pltpu.make_async_remote_copy(
            src_ref=src, dst_ref=dst, send_sem=ssem, recv_sem=rsem, device_id=(row, col), device_id_type=MESH
        )

    def part(k):
        return pl.ds(offs[k], cuts[k])

    def span(g):
        return pl.ds(offs[firsts[g]], wide[g])

    def got(ref, sem):
        remote(ref, ref, sem, sem, r, sib).wait_recv()

    def sent(ref, sem):
        remote(ref, ref, sem, sem, r, sib).wait_send()

    barrier = pltpu.get_barrier_semaphore()

    def greet(row, col):
        pl.semaphore_signal(barrier, inc=1, device_id=(row, col), device_id_type=MESH)

    for i in range(1, M):
        greet(r, (m + i) % M)
    for i in range(1, R):
        greet((r + i) % R, m)

    @pl.when(jnp.logical_not(home))
    def _():
        for i in range(1, R):
            greet((r + i) % R, 2 * r + c)

    in_gain.start()
    in_bias.start()
    pltpu.make_async_copy(win_hbm, win, wsem.at[0]).start()
    pltpu.make_async_copy(wout_hbm, wout, wsem.at[1]).start()
    in_tok.wait()
    own = tok[...].astype(F32)
    lane = lax.broadcasted_iota(jnp.int32, (height, 128), 1)
    s1 = jnp.sum(own, axis=1, keepdims=True)
    s2 = jnp.sum(own * own, axis=1, keepdims=True)
    stc[m] = jnp.where(lane == 0, s1, s2).T[0:8]

    pl.semaphore_wait(barrier, (M - 1) + (R - 1) + jnp.where(home, 0, R - 1))

    toward = 2 * (z // 2) - 1

    def c_a(k, i):
        zd = (z + i * toward + Z) % Z
        return remote(tok.at[span(k)], xs.at[c, r, span(k)], (s_a if i else s_ap).at[0], r_a.at[k], z, 2 * zd + c)

    def c_sib(k, t, src):
        return remote(src, xs.at[c, t, span(k)], s_sib.at[0], r_sib.at[k], r, sib)

    def c_st(i):
        return remote(stc.at[m], stc.at[m], s_st.at[0], r_st.at[0], r, (m + i) % M)

    def c_mi(i):
        return remote(mi.at[r], mi.at[r], s_mi.at[0], r_mi.at[0], peers[i], m)

    def c_r1(k, h, i):
        tile = (first[h], rd)[i]
        return remote(
            pbuf.at[h, :, tile, part(k)], r1.at[h, i, :, part(k)], s_b.at[0], (r_q, r_p)[i].at[k, h], first[h], m
        )

    def c_r1_half(k, h, i, j):
        tile = (first[h], rd)[i]
        return remote(
            pbuf.at[h, j, tile, part(k)], r1.at[h, i, j, part(k)], s_b.at[0], (r_q, r_p)[i].at[k, h], first[h], m
        )

    def c_r2(k, h):
        return remote(qbuf.at[h, part(k)], r2.at[h, part(k)], s_f.at[0], r_q.at[k, h], second[h], m)

    def c_ag(k, h, i):
        tile = (r, r, second[h])[i]
        to = (second[h], first[h], first[h])[i]
        ref = hid.at[h, tile, part(k)]
        return remote(ref, ref, (s_b, s_b, s_f)[i].at[0], r_g.at[k, h] if i == 0 else r_ag.at[k], to, m)

    def c_os(k):
        return remote(osend.at[:, span(k)], osib.at[:, span(k)], s_os.at[0], r_os.at[k], r, sib)

    def c_cm(k, i):
        t = peers[i]
        return remote(csend.at[t, span(k)], cmid.at[r, span(k)], s_cm.at[0], r_cm.at[k], t, m)

    def c_cz(k, q, src):
        return remote(src, crecv.at[z, span(k)], s_cz.at[0], r_cz.at[k], r, 2 * q + c)

    def plane_of(k, t):
        return (k + t) % Z

    def tile_of(k):
        return (z + Z * k - k) % Z

    def c_ax(k, i, src):
        t = tile_of(k)
        zd = (z + i * toward + Z) % Z
        return remote(src, xs.at[c, t, span(k)], s_ax.at[0], r_a.at[k], r, 2 * zd + c)

    def c_a1(k):
        return remote(
            tok.at[span(k)], xs.at[c, r, span(k)], s_af.at[far_in.index(k)], r_af.at[far_in.index(k)], z,
            2 * plane_of(k, r) + c,
        )

    def keeps(k):
        return home & (plane_of(k, r) == z)

    def c_cx(k, i):
        zd = (z + i * toward + Z) % Z
        t = (zd + Z * k - k) % Z
        return remote(csend.at[t, span(k)], crecv.at[z, span(k)], s_cz.at[0], r_cz.at[k], r, 2 * zd + c)

    def c_cp(k):
        return remote(cfin.at[span(k)], cmid.at[r, span(k)], s_cp.at[far_out.index(k)], r_cm.at[k], tile_of(k), m)

    def c_fin(k, q, src):
        j = far_out.index(k)
        return remote(src, fin.at[span(k)], s_fin.at[j], r_fin.at[j], r, 2 * q + c)

    def stage_send(k):
        if k in far_in:
            @pl.when(keeps(k))
            def _():
                xs[c, r, span(k)] = tok[span(k)]

            @pl.when(jnp.logical_not(keeps(k)))
            def _():
                c_a1(k).start()

            return
        for i in (1, 3, 2):
            c_a(k, i).start()

        @pl.when(home)
        def _():
            xs[c, r, span(k)] = tok[span(k)]
            c_sib(k, r, tok.at[span(k)]).start()

        @pl.when(jnp.logical_not(home))
        def _():
            c_a(k, 0).start()

    def stage_st0(_):
        for i in range(1, M):
            c_st(i).start()

    def stage_st1(_):
        got(stc.at[0:M - 1], r_st.at[0])
        tot = stc[0]
        for q in range(1, M):
            tot = tot + stc[q]
        mean = tot[0:1] / D
        var = jnp.maximum(tot[1:2] / D - mean * mean, 0.0)
        inv = lax.rsqrt(var + floor_value)
        sub = lax.broadcasted_iota(jnp.int32, (8, height), 0)
        mi[r] = jnp.where(sub == 0, mean, inv)
        for i in range(3):
            c_mi(i).start()

    def stage_st2(_):
        got(mi.at[0:R - 1], r_mi.at[0])
        sub = lax.broadcasted_iota(jnp.int32, (128, height), 0)
        for t in range(R):
            colst[t] = jnp.where(sub == 0, mi[t, 0:1], mi[t, 1:2]).T

    def stage_a1(k):
        if k not in far_in:
            return
        t = tile_of(k)

        def spread(src):
            for i in (1, 3, 2):
                c_ax(k, i, src).start()
            c_sib(k, t, src).start()

        @pl.when(keeps(k))
        def _():
            spread(tok.at[span(k)])

        @pl.when(jnp.logical_not(keeps(k)))
        def _():
            got(xs.at[c, t, span(k)], r_af.at[far_in.index(k)])
            spread(xs.at[c, t, span(k)])

    def stage_a(k):
        if k in far_in:
            got(xs.at[c, 0:R - 1, span(k)], r_a.at[k])
            for i in range(1, R):
                t = (tile_of(k) + i) % R
                c_sib(k, t, xs.at[c, t, span(k)]).start()
            return

        @pl.when(home)
        def _():
            got(xs.at[c, 0:R - 1, span(k)], r_a.at[k])

        @pl.when(jnp.logical_not(home))
        def _():
            got(xs.at[c, :, span(k)], r_a.at[k])
            c_sib(k, r, xs.at[c, r, span(k)]).start()

        for i in range(1, R):
            t = (r + i) % R
            c_sib(k, t, xs.at[c, t, span(k)]).start()

    def stage_m1(k):
        n = wide[k]
        got(xs.at[1 - c, :, span(k)], r_sib.at[k])
        if k == 0:
            in_gain.wait()
        stats = colst[:, span(k)].reshape(R * n, 128)
        mean_c, inv_c = stats[:, 0:1], stats[:, 1:2]
        for cc in range(2):
            x = xs[cc, :, span(k)].astype(F32).reshape(R * n, width)
            nx[cc, 0:R * n] = ((x - mean_c) * inv_c * gain[2 * r + cc]).astype(BF16)

        if k == 0:
            pltpu.make_async_copy(win_hbm, win, wsem.at[0]).wait()
            in_bias.wait()

        tile = half // 2

        def columns(h, j):
            wat = pl.multiple_of(h * half + j * tile, 128)
            acc = jnp.dot(nx[0, 0:R * n], win[0:width, pl.ds(wat, tile)], preferred_element_type=F32)
            acc += jnp.dot(nx[1, 0:R * n], win[width:2 * width, pl.ds(wat, tile)], preferred_element_type=F32)
            pbuf[h, j, :, span(k)] = acc.astype(BF16).reshape(R, n, tile)

        if k < SPLIT:
            for j in range(2):
                for h in range(2):
                    columns(h, j)
                    for sub in subs[k]:
                        c_r1_half(sub, h, 1, j).start()
                        c_r1_half(sub, h, 0, j).start()
            return

        for h in range(2):
            def col(j, _):
                columns(h, j)
                return 0

            lax.fori_loop(0, 2, col, 0)
            for sub in subs[k]:
                c_r1(sub, h, 1).start()
                c_r1(sub, h, 0).start()

    def stage_b1(k):
        for h in range(2):
            got(r1.at[h, 1, :, part(k)], r_p.at[k, h])
            for j in range(2):
                mine = pbuf[h, j, second[h], part(k)].astype(F32)
                cols = slice(j * (half // 2), (j + 1) * (half // 2))
                qbuf[h, part(k), cols] = (mine + r1[h, 1, j, part(k)].astype(F32)).astype(BF16)
            c_r2(k, h).start()

    def stage_b2(k):
        for h in range(2):
            got(r1.at[h, :, :, part(k)], r_q.at[k, h])
            for j in range(2):
                cols = slice(j * (half // 2), (j + 1) * (half // 2))
                pre = pbuf[h, j, r, part(k)].astype(F32) + r1[h, 0, j, part(k)].astype(F32)
                pre = pre + r2[h, part(k), cols].astype(F32)
                at = h * half + j * (half // 2)
                pre = pre + bias[0:1, at:at + half // 2]
                hid[h, r, part(k), cols] = gelu(pre).astype(BF16)
            c_ag(k, h, 0).start()
            c_ag(k, h, 1).start()

    def stage_b3(k):
        for h in range(2):
            got(hid.at[h, second[h], part(k)], r_g.at[k, h])
            c_ag(k, h, 2).start()

    def stage_b4(k):
        n = wide[k]
        for sub in subs[k]:
            got(hid.at[:, 0:2, part(sub)], r_ag.at[sub])

        if ("b4", k) == next(stage for stage in order if stage[0] == "b4"):
            pltpu.make_async_copy(wout_hbm, wout, wsem.at[1]).wait()

        def product(cc):
            at = pl.multiple_of(cc * width, 128)
            acc = None
            for h in range(2):
                a = hid[h, :, span(k)].reshape(R * n, half)
                term = jnp.dot(a, wout[h * half:(h + 1) * half, pl.ds(at, width)], preferred_element_type=F32)
                acc = term if acc is None else acc + term
            return acc.reshape(R, n, width)

        osend[:, span(k)] = product(1 - c).astype(BF16)
        c_os(k).start()
        oown[:, span(k)] = product(c)

    def stage_c1(k):
        c_os(k).wait_recv()
        if k in far_out:
            t = tile_of(k)
            csend[:, span(k)] = (oown[:, span(k)] + osib[:, span(k)].astype(F32)).astype(BF16)
            for i in (1, 3, 2):
                c_cx(k, i).start()
            oown[t, span(k)] = oown[t, span(k)] + osib[t, span(k)].astype(F32)
            return
        csend[:, span(k)] = (oown[:, span(k)] + osib[:, span(k)].astype(F32)).astype(BF16)
        for i in range(3):
            c_cm(k, i).start()

        @pl.when(jnp.logical_not(home))
        def _():
            c_cz(k, r, csend.at[r, span(k)]).start()

    def stage_c2(k):
        if k in far_out:
            t = tile_of(k)
            total = oown[t, span(k)]
            got(crecv.at[0:Z - 1, span(k)], r_cz.at[k])
            for i in range(1, Z):
                q = (z + i) % Z
                total = total + crecv[q, span(k)].astype(F32)
            cfin[span(k)] = total.astype(BF16)

            @pl.when(t != r)
            def _():
                c_cp(k).start()

            return
        got(cmid.at[0:R - 1, span(k)], r_cm.at[k])
        for i in range(3):
            q = peers[i]

            @pl.when(q != z)
            def _():
                c_cz(k, q, cmid.at[q, span(k)]).start()

    def stage_c4(k):
        if k not in far_out:
            return

        @pl.when(tile_of(k) == r)
        def _():
            @pl.when(jnp.logical_not(home))
            def _():
                c_fin(k, r, cfin.at[span(k)]).start()

            got(cmid.at[0:R - 1, span(k)], r_cm.at[k])
            for i in range(3):
                q = peers[i]

                @pl.when(q != z)
                def _():
                    c_fin(k, q, cmid.at[q, span(k)]).start()

    def stage_c3(k):
        if k in far_out:
            mine = tile_of(k) == r

            @pl.when(mine & home)
            def _():
                fin[span(k)] = cfin[span(k)]

            @pl.when(mine & jnp.logical_not(home))
            def _():
                fin[span(k)] = cmid[z, span(k)]

            @pl.when(jnp.logical_not(mine))
            def _():
                got(fin.at[span(k)], r_fin.at[far_out.index(k)])

            out[span(k)] = (tok[span(k)].astype(F32) + fin[span(k)].astype(F32)).astype(BF16)
            return

        @pl.when(home)
        def _():
            crecv[z, span(k)] = csend[r, span(k)]

        @pl.when(jnp.logical_not(home))
        def _():
            crecv[z, span(k)] = cmid[z, span(k)]

        got(crecv.at[0:Z - 1, span(k)], r_cz.at[k])
        total = (crecv[0, span(k)].astype(F32) + crecv[1, span(k)].astype(F32)) + (
            crecv[2, span(k)].astype(F32) + crecv[3, span(k)].astype(F32)
        )
        out[span(k)] = (tok[span(k)].astype(F32) + total).astype(BF16)

    def stage_e(_):
        near = sum(wide[k] for k in range(G) if k not in far_in)
        sent(xs.at[0, 0:Z - 1, 0:near], s_a.at[0])
        sent(xs.at[0, 0:Z - 1, near:height], s_ax.at[0])

        @pl.when(jnp.logical_not(home))
        def _():
            sent(tok.at[0:near], s_ap.at[0])

        for k in far_in:
            @pl.when(jnp.logical_not(keeps(k)))
            def _():
                c_a1(k).wait_send()

        sent(xs.at[0], s_sib.at[0])
        sent(stc.at[0:M - 1], s_st.at[0])
        sent(mi.at[0:R - 1], s_mi.at[0])
        sent(hid, s_b.at[0])
        sent(hid.at[:, 0:2], s_f.at[0])
        sent(osend, s_os.at[0])
        sent(csend.at[0:R - 1, 0:sum(wide[k] for k in range(G) if k not in far_out)], s_cm.at[0])
        for k in far_out:
            @pl.when(tile_of(k) != r)
            def _():
                c_cp(k).wait_send()

            @pl.when(tile_of(k) == r)
            def _():
                sent(crecv.at[0:Z - 1, span(k)], s_fin.at[far_out.index(k)])

        sent(crecv.at[0:Z - 1], s_cz.at[0])

    stages = {
        "send": stage_send, "st0": stage_st0, "st1": stage_st1, "st2": stage_st2, "a1": stage_a1, "a": stage_a,
        "m1": stage_m1, "b1": stage_b1, "b2": stage_b2, "b3": stage_b3, "b4": stage_b4, "c1": stage_c1,
        "c2": stage_c2, "c4": stage_c4, "c3": stage_c3, "e": stage_e,
    }
    assert len(set(order)) == len(order)
    for name, k in order:
        stages[name](k)


ORDER = (
    "st0_0 send_0 send_1",
    "send_2 send_3 send_4",
    "send_5 st1_0 a_0",
    "st2_0 m1_0 a_1",
    "m1_1 b1_0 a1_2",
    "b1_1 a1_5 a1_3",
    "a1_4 b2_0 b2_1",
    "a_2 m1_2 b3_0",
    "b1_2 b3_1 a_5",
    "a_3 m1_3 b2_2",
    "a_4 m1_4 b4_1",
    "c1_1 b1_3 b3_2",
    "m1_5 b1_4 b2_3",
    "b4_0 b4_2 c1_0",
    "b1_5 c1_2 b2_4",
    "b3_3 b2_5 b3_4",
    "c2_0 c2_1 b4_3",
    "c1_3 b3_5 c2_2",
    "b4_4 c4_0 c1_4",
    "b4_5 c4_1 c2_3",
    "c1_5 c4_2 c2_4",
    "c3_0 c4_3 c2_5",
    "c3_4 c3_1 c3_2",
    "c3_3 c3_5 e_0",
)


def schedule():
    names = " ".join(ORDER).split()
    return [(name.split("_")[0], int(name.split("_")[1])) for name in names]


def fused(tokens, norm_gain, hidden_bias, weight_in, weight_out, R, M, D):
    height, width = tokens.shape
    depth, ff = weight_in.shape
    half = ff // 2
    step = height // sum(sum(group) for group in UNITS)
    groups = [[u * step for u in group] for group in UNITS]
    K, G = sum(len(group) for group in groups), len(groups)
    V = pltpu.VMEM
    S = pltpu.SemaphoreType.DMA
    vm = pl.BlockSpec(memory_space=pltpu.VMEM)
    hbm = pl.BlockSpec(memory_space=pltpu.HBM)
    return pl.pallas_call(
        functools.partial(kernel, R, M, D, groups, schedule(), FAR_IN, FAR_OUT),
        out_shape=pltpu.VMEM(tokens.shape, BF16),
        in_specs=[hbm, hbm, hbm, hbm, hbm],
        out_specs=vm,
        scratch_shapes=[
            V(tokens.shape, BF16), V((M, 1, width), F32), V((1, ff), F32), V(weight_in.shape, BF16), V(weight_out.shape, BF16),
            V((2, R, height, width), BF16), V((2, R * max(sum(group) for group in groups), width), BF16),
            V((M, 8, height), F32), V((R, 8, height), F32), V((R, height, 128), F32),
            V((2, 2, R, height, half // 2), BF16), V((2, 2, 2, height, half // 2), BF16), V((2, height, half), BF16),
            V((2, height, half), BF16), V((2, R, height, half), BF16),
            V((R, height, width), BF16), V((R, height, width), BF16), V((R, height, width), F32),
            V((R, height, width), BF16), V((R, height, width), BF16), V((R, height, width), BF16),
            V((height, width), BF16), V((height, width), BF16), S((5,)),
            S((1,)), S((1,)), S((len(FAR_IN),)), S((1,)), S((G,)), S((len(FAR_IN),)), S((1,)), S((G,)), S((1,)), S((1,)),
            S((1,)), S((1,)), S((1,)), S((1,)), S((K, 2)), S((K, 2)), S((K, 2)), S((K,)),
            S((1,)), S((G,)), S((1,)), S((len(FAR_OUT),)), S((G,)), S((1,)), S((G,)), S((len(FAR_OUT),)), S((len(FAR_OUT),)),
        ],
        compiler_params=pltpu.CompilerParams(
            collective_id=0, has_side_effects=True, vmem_limit_bytes=60 * 1024 * 1024
        ),
    )(tokens, norm_gain.reshape(M, 1, width), hidden_bias.reshape(1, ff), weight_in, weight_out)


def plain(tokens, norm_gain, hidden_bias, weight_in, weight_out, R, M, D):
    as_float = tokens.astype(F32)
    moment_sum, square_sum = lax.psum((jnp.sum(as_float, axis=1), jnp.sum(as_float * as_float, axis=1)), "mp")
    width = tokens.shape[1]
    gain = lax.dynamic_slice_in_dim(norm_gain, lax.axis_index("mp") * width, width)
    mean = moment_sum / D
    inverse = lax.rsqrt(jnp.maximum(square_sum / D - mean * mean, 0.0) + floor_value)
    part = ((as_float - mean[:, None]) * inverse[:, None] * gain[None, :]).astype(BF16)
    normed = lax.all_gather(part, "mp", axis=1, tiled=True)
    shuffled = lax.all_to_all(normed, "rows", split_axis=1, concat_axis=0, tiled=True)
    preact = lax.psum_scatter(
        jnp.dot(shuffled, weight_in, preferred_element_type=F32), "rows", scatter_dimension=0, tiled=True
    )
    hidden = jax.nn.gelu(preact + hidden_bias[None, :], approximate=False).astype(BF16)
    hidden = lax.all_gather(hidden, "rows", axis=0, tiled=True)
    terms = jnp.dot(hidden, weight_out, preferred_element_type=F32)
    terms = lax.all_to_all(terms, "rows", split_axis=0, concat_axis=1, tiled=True)
    branch = lax.psum_scatter(terms, "mp", scatter_dimension=1, tiled=True)
    return (as_float + branch).astype(BF16)


def solution(mesh):
    R, M = mesh.shape["rows"], mesh.shape["mp"]

    def body(tokens, norm_gain, hidden_bias, weight_in, weight_out):
        D = norm_gain.shape[0]
        aligned = tokens.shape[1] % 128 == 0 and weight_in.shape[1] % 512 == 0 and tokens.shape[0] == 16 * sum(sum(group) for group in UNITS)
        if R == 4 and M == 2 * R and aligned and tokens.shape[0] % 128 == 0:
            return fused(tokens, norm_gain, hidden_bias, weight_in, weight_out, R, M, D)
        return plain(tokens, norm_gain, hidden_bias, weight_in, weight_out, R, M, D)

    return jax.shard_map(
        body,
        mesh=mesh,
        in_specs=(P("rows", "mp"), P(), P("mp"), P("rows", "mp"), P("mp", "rows")),
        out_specs=P("rows", "mp"),
        check_vma=False,
    )
```
